256 devices in a mesh: prow: 16 (over y, x), pcol: 16 (over z, core).
Axes of the slice: x: 4, y: 4, z: 8, core: 2. Of those that a mesh axis runs over, the one named last changes fastest.
Arguments:
- matrix: float32 [4, 16, 256, 4, 16, 256], P(None, 'prow', None, None, 'pcol'), may hold values from -6 to 6, as said below
- factor: float32 [4, 16, 256, 4, 16, 256], P(None, 'prow', None, None, 'pcol'), may hold values from -3 to 3, as said below
Outputs:
- reduced: float32 [4, 16, 256, 4, 16, 256], P(None, 'prow', None, None, 'pcol')
The draws below stay inside these ranges and needn't reach their ends.
Inputs may be any that keep to these rules, and one draw needn't show every extreme that they name: Symmetric matrix stored in its lower triangle: every entry above the diagonal is zero. `factor`: lower triangular with diagonal entries between 1 and 3; every entry above the diagonal is zero.
All inputs are finite; a program needn't handle non-finite values.
Results may differ from the reference program's by a relative error of at most 0.0001.
Values sent between devices are 32-bit elements; how exact they have to be, the bound alone decides.
No kernel may reach another device: no remote copies, remote signals or barrier semaphores. Data moves between devices by JAX's collectives and lax.ppermute only.
A program may use at most 128 MiB of HBM per device.

```python
import jax
import jax.numpy as jnp
from jax import lax

ORDER = 16384
NB = 256
BLOCKS = 2
RT = 4
CT = 4


def draw_matrix(key, part):
    rows = jnp.arange(ORDER, dtype=jnp.int32)[:, None]
    cols = jnp.arange(ORDER, dtype=jnp.int32)[None, :]
    values = jnp.clip(jax.random.normal(key, (ORDER, ORDER), jnp.float32), -6.0, 6.0)
    values = jnp.where(rows >= cols, values, 0.0)
    return values.reshape(RT, ORDER // (RT * NB), NB, CT, ORDER // (CT * NB), NB)


def draw_factor(key, part):
    first, second = jax.random.split(jax.random.fold_in(key, 7))
    rows = jnp.arange(ORDER, dtype=jnp.int32)[:, None]
    cols = jnp.arange(ORDER, dtype=jnp.int32)[None, :]
    same_tile = rows // NB == cols // NB
    spread = jnp.where(same_tile, 0.5, 0.3) / jnp.sqrt(jnp.float32(NB))
    noise = jnp.clip(jax.random.normal(first, (ORDER, ORDER), jnp.float32), -5.0, 5.0)
    diagonal = jnp.exp(jax.random.uniform(second, (ORDER,), jnp.float32, 0.0, jnp.log(3.0)))
    values = jnp.where(rows > cols, noise * spread, 0.0) + jnp.where(rows == cols, diagonal[:, None], 0.0)
    return values.reshape(RT, ORDER // (RT * NB), NB, CT, ORDER // (CT * NB), NB)


def setup_inputs(seed: int = 0) -> dict:
    keys = jax.random.split(jax.random.key(seed), 3)
    return {
        "matrix": draw_matrix(jax.random.fold_in(keys[2], 71), 0),
        "factor": draw_factor(jax.random.fold_in(keys[2], 71), 0),
    }


highest = lax.Precision.HIGHEST

def product(left, right):
    return jnp.dot(left.astype(jnp.float32), right.astype(jnp.float32), precision=highest, preferred_element_type=jnp.float32)

def product_trans(left, right):
    return lax.dot_general(left.astype(jnp.float32), right.astype(jnp.float32), (((1,), (1,)), ((), ())), precision=highest, preferred_element_type=jnp.float32)

def diagonal_core(diag_block, diag_factor, width):
    identity = jnp.eye(width, dtype=jnp.float32)
    inverse = lax.linalg.triangular_solve(diag_factor, identity, left_side=True, lower=True)
    symmetric = diag_block + diag_block.T - jnp.diag(jnp.diagonal(diag_block))
    inner = product_trans(product(inverse, symmetric), inverse)
    return (inverse, 0.5 * (inner + inner.T))

def reference(matrix, factor):
    full = matrix.reshape(ORDER, ORDER)
    lower = factor.reshape(ORDER, ORDER)
    for step in range(BLOCKS):
        low = step * NB
        high = low + NB
        inverse, core = diagonal_core(full[low:high, low:high], lower[low:high, low:high], NB)
        panel = full[high:, low:high]
        factor_panel = lower[high:, low:high]
        shared = product(factor_panel, core)
        halfway = product_trans(panel, inverse) - 0.5 * shared
        finished = halfway - 0.5 * shared
        update = product_trans(halfway, factor_panel) + product_trans(factor_panel, halfway)
        trailing = full[high:, high:] - jnp.tril(update)
        full = full.at[high:, high:].set(trailing)
        full = full.at[low:high, low:high].set(jnp.tril(core))
        full = full.at[high:, low:high].set(finished)
    return full.reshape(RT, ORDER // (RT * NB), NB, CT, ORDER // (CT * NB), NB)
```

```python
import jax
import jax.numpy as jnp
from jax import lax
from jax.experimental import pallas as pl
from jax.experimental.pallas import tpu as pltpu
from jax.sharding import Mesh
from jax.sharding import PartitionSpec as P

NB = 256
ROW = ("y", "x")
COL = ("z", "core")
SLABS = 8
SLAB = NB // SLABS


NT = (((1,), (1,)), ((), ()))
NN = (((1,), (0,)), ((), ()))


def full(left, right, dims=NT):
    return lax.dot_general(left, right, dims, precision=lax.Precision.HIGHEST, preferred_element_type=jnp.float32)


def split(value):
    high = value.astype(jnp.bfloat16)
    return high, (value - high.astype(jnp.float32)).astype(jnp.bfloat16)


def three(left, right):
    def dot(a, b):
        return lax.dot_general(a, b, NT, preferred_element_type=jnp.float32)

    return dot(left[0], right[0]) + dot(left[0], right[1]) + dot(left[1], right[0])


def pack_kernel(matrix, factor, *rest):
    pieces, sems = rest[:SLABS], rest[SLABS]
    copies = []
    for slab in range(SLABS):
        for m, source in enumerate((matrix, factor)):
            for tile in range(4):
                for half in range(2):
                    copies.append(
                        pltpu.make_async_copy(
                            source.at[tile, 0, pl.ds(slab * SLAB, SLAB), 0, :, pl.ds(half * 128, 128)],
                            pieces[slab].at[pl.ds(((m * 4 + tile) * 2 + half) * SLAB, SLAB)],
                            sems.at[len(copies)],
                        )
                    )
    for copy in copies:
        copy.start()
    for copy in copies:
        copy.wait()


def pack(matrix, factor):
    count = SLABS * 16
    return pl.pallas_call(
        pack_kernel,
        in_specs=[pl.BlockSpec(memory_space=pl.ANY)] * 2,
        out_specs=[pl.BlockSpec(memory_space=pl.ANY)] * SLABS,
        out_shape=[jax.ShapeDtypeStruct((16 * SLAB, 1, 128), jnp.float32)] * SLABS,
        scratch_shapes=[pltpu.SemaphoreType.DMA((count,))],
        name="pack",
    )(matrix, factor)


def iotas():
    return (
        lax.broadcasted_iota(jnp.int32, (NB, NB), 0),
        lax.broadcasted_iota(jnp.int32, (NB, NB), 1),
    )


def inverse(lower, rows, cols):
    eye = rows == cols
    recip = 1.0 / jnp.sum(jnp.where(eye, lower, 0.0), axis=1, keepdims=True)
    recip_row = 1.0 / jnp.sum(jnp.where(eye, lower, 0.0), axis=0, keepdims=True)
    pair = (rows // 2 == cols // 2) & (rows > cols)
    result = jnp.where(eye, recip, 0.0) - jnp.where(pair, lower * recip * recip_row, 0.0)
    size = 2
    while size < NB:
        band = (rows // (2 * size) == cols // (2 * size)) & (rows // size > cols // size)
        block = jnp.where(band, lower, 0.0)
        result = result - full(full(result, block, NN), result, NN)
        size *= 2
    return result


def head_kernel(head, v0, s0, v1, s1, h0, l10):
    rows, cols = iotas()
    eye = rows == cols

    def tile(core, row, m):
        return jnp.concatenate([head[:, core, row, m, half].reshape(NB, 128) for half in range(2)], axis=1)

    a00, l00, a10, low, a11, l11 = (
        tile(0, 0, 0), tile(0, 0, 1), tile(0, 1, 0), tile(0, 1, 1), tile(1, 1, 0), tile(1, 1, 1),
    )
    inv0 = inverse(l00, rows, cols)
    inv1 = inverse(l11, rows, cols)
    part = full(full(inv0, jnp.where(eye, 0.5 * a00, a00), NN), inv0)
    core0 = part + part.T
    half0 = full(a10, inv0) - 0.5 * full(low, core0)
    inner = jnp.where(eye, 0.5 * a11, a11) - full(half0, low)
    part = full(full(inv1, inner, NN), inv1)
    core1 = part + part.T
    v0[...] = inv0
    s0[...] = core0
    v1[...] = inv1
    s1[...] = core1
    h0[...] = half0
    l10[...] = low


def head_math(head):
    return pl.pallas_call(
        head_kernel,
        out_shape=[jax.ShapeDtypeStruct((NB, NB), jnp.float32)] * 6,
        compiler_params=pltpu.CompilerParams(vmem_limit_bytes=40 * 2**20),
        name="head",
    )(head)


def main_kernel(place, raw_row, raw_col, v0, s0, v1, s1, h0, l10, local, out, col_hi, col_lo, head_hi, head_lo):
    step = pl.program_id(0)
    p = place[0]
    c = place[1]

    def read(raw, core, m, tile):
        return jnp.concatenate([raw[:, core, m, tile, half].reshape(NB, 128) for half in range(2)], axis=1)

    def panels(raw, tile):
        def head(k):
            return head_hi[k], head_lo[k]

        a0, a1 = read(raw, 0, 0, tile), read(raw, 1, 0, tile)
        f0, f1 = split(read(raw, 0, 1, tile)), split(read(raw, 1, 1, tile))
        p0 = three(f0, head(1))
        half0 = three(split(a0), head(0)) - 0.5 * p0
        g0 = split(half0)
        a1 = a1 - three(g0, head(5)) - three(f0, head(4))
        p1 = three(f1, head(3))
        half1 = three(split(a1), head(2)) - 0.5 * p1
        g1 = split(half1)
        return g0, f0, g1, f1, half0 - 0.5 * p0, half1 - 0.5 * p1

    @pl.when(step == 0)
    def _():
        for k, ref in enumerate((v0, s0, v1, s1, h0, l10)):
            head_hi[k], head_lo[k] = split(ref[...])

        def one(tile, carry):
            g0, f0, g1, f1, _, _ = panels(raw_col, tile)
            for k, (hi, lo) in enumerate((f0, g0, f1, g1)):
                col_hi[tile, :, k * NB : (k + 1) * NB] = hi
                col_lo[tile, :, k * NB : (k + 1) * NB] = lo
            return carry

        lax.fori_loop(0, 4, one, 0)

    g0, f0, g1, f1, done0, done1 = panels(raw_row, step)
    row_hi = jnp.concatenate([g0[0], f0[0], g1[0], f1[0]], axis=1)
    row_lo = jnp.concatenate([g0[1], f0[1], g1[1], f1[1]], axis=1)
    rows, cols = iotas()

    def put(tile, value):
        for half in range(2):
            out[pl.ds(tile * 2 + half, NB, stride=8), :] = value[:, half * 128 : (half + 1) * 128]

    def get(tile):
        return jnp.concatenate([local[pl.ds(tile * 2 + half, NB, stride=8), :] for half in range(2)], axis=1)

    for tile in range(4):
        below = (step > tile) | ((step == tile) & (p > c))
        same = (step == tile) & (p == c)
        special = (c < 2) if tile == 0 else False

        @pl.when((below | same) & jnp.logical_not(special))
        def _():
            update = three((row_hi, row_lo), (col_hi[tile], col_lo[tile]))
            keep = jnp.logical_or(below, rows >= cols)
            put(tile, get(tile) - jnp.where(keep, update, 0.0))

        @pl.when(jnp.logical_not(below | same))
        def _():
            put(tile, get(tile))

        if tile == 0:

            @pl.when(below & (c == 0))
            def _():
                put(0, done0)

            @pl.when(below & (c == 1))
            def _():
                put(0, done1)

            @pl.when(same & (c == 0))
            def _():
                put(0, jnp.where(rows >= cols, s0[...], 0.0))

            @pl.when(same & (c == 1))
            def _():
                put(0, jnp.where(rows >= cols, s1[...], 0.0))


def main_math(place, raw_row, raw_col, head, local):
    def whole(shape):
        return pl.BlockSpec(shape, lambda i: (0,) * len(shape))

    raw = (SLABS, 2, 2, 4, 2, SLAB, 128)
    block = pl.BlockSpec((2048, 128), lambda i: (i, 0))
    return pl.pallas_call(
        main_kernel,
        grid=(4,),
        in_specs=[pl.BlockSpec(memory_space=pltpu.SMEM), whole(raw), whole(raw)] + [whole((NB, NB))] * 6 + [block],
        out_specs=block,
        out_shape=jax.ShapeDtypeStruct((8192, 128), jnp.float32),
        scratch_shapes=[
            pltpu.VMEM((4, NB, 4 * NB), jnp.bfloat16),
            pltpu.VMEM((4, NB, 4 * NB), jnp.bfloat16),
            pltpu.VMEM((6, NB, NB), jnp.bfloat16),
            pltpu.VMEM((6, NB, NB), jnp.bfloat16),
        ],
        compiler_params=pltpu.CompilerParams(vmem_limit_bytes=56 * 2**20),
        name="main",
    )(place, raw_row.reshape(raw), raw_col.reshape(raw), *head, local)


def on_device(matrix, factor):
    z = lax.axis_index("z")
    p = lax.axis_index(ROW)
    c = lax.axis_index(COL)
    pieces = [piece.reshape(16 * SLAB, 128) for piece in pack(matrix, factor)]
    order = (4, 1, 7, 2, 6, 3, 5)
    got = [lax.ppermute(pieces[k], "z", [(0, k)]) for k in order]
    total = got[0]
    for value in got[1:]:
        total = total + value
    mine = jnp.where(z == 0, pieces[0], total)
    top = mine.reshape(2, 4, 2 * SLAB, 128)[:, 0].reshape(4 * SLAB, 128)
    tops = lax.all_gather(top, ROW)[:2].reshape(8 * SLAB, 128)
    head = lax.all_gather(tops, COL).reshape(SLABS, 2, 2, 2, 2, SLAB, 128)
    swapped = lax.ppermute(mine, ROW + COL, [(r * 16 + j, j * 16 + r) for r in range(16) for j in range(16)])
    raw_row = lax.all_gather(mine, COL)
    raw_col = lax.all_gather(swapped, ROW)
    result = main_math(jnp.stack([p, c]), raw_row, raw_col, head_math(head), matrix.reshape(8192, 128))
    return result.reshape(matrix.shape)


def solution(mesh):
    torus = Mesh(mesh.devices.reshape(4, 4, 8, 2), ("y", "x", "z", "core"))
    spec = P(None, ROW, None, None, COL, None)
    return jax.shard_map(on_device, mesh=torus, in_specs=(spec, spec), out_specs=spec, check_vma=False)
```

```python
import jax
import jax.numpy as jnp
from jax import lax
from jax.experimental import pallas as pl
from jax.experimental.pallas import tpu as pltpu
from jax.sharding import Mesh
from jax.sharding import PartitionSpec as P

NB = 256
ROW = ("y", "x")
COL = ("z", "core")
SLABS = 8
SLAB = NB // SLABS


NT = (((1,), (1,)), ((), ()))
NN = (((1,), (0,)), ((), ()))


def full(left, right, dims=NT):
    return lax.dot_general(left, right, dims, precision=lax.Precision.HIGHEST, preferred_element_type=jnp.float32)


def split(value):
    high = value.astype(jnp.bfloat16)
    return high, (value - high.astype(jnp.float32)).astype(jnp.bfloat16)


def three(left, right):
    def dot(a, b):
        return lax.dot_general(a, b, NT, preferred_element_type=jnp.float32)

    return dot(left[0], right[0]) + dot(left[0], right[1]) + dot(left[1], right[0])


def pack_kernel(place, matrix, factor, *rest):
    pieces, (buffer, sems) = rest[:SLABS], rest[SLABS:]

    @pl.when(place[2] == 0)
    def _():
        copies = {}
        for tile in range(4):
            for m, source in enumerate((matrix, factor)):
                rows = pl.ds(tile * 8 * NB, 8 * NB)
                copies[tile, m] = pltpu.make_async_copy(source.at[rows], buffer.at[m, rows], sems.at[m * 4 + tile])
                copies[tile, m].start()
        for tile in range(4):
            for m in range(2):
                copies[tile, m].wait()
                for half in range(2):
                    for slab in range(SLABS):
                        value = buffer[m, pl.ds((tile * NB + slab * SLAB) * 8 + half, SLAB, stride=8), :]
                        pieces[slab][pl.ds(((m * 4 + tile) * 2 + half) * SLAB, SLAB), :] = value


def pack(place, matrix, factor):
    return pl.pallas_call(
        pack_kernel,
        in_specs=[pl.BlockSpec(memory_space=pltpu.SMEM)] + [pl.BlockSpec(memory_space=pl.ANY)] * 2,
        out_specs=[pl.BlockSpec(memory_space=pltpu.VMEM)] * SLABS,
        out_shape=[jax.ShapeDtypeStruct((16 * SLAB, 128), jnp.float32)] * SLABS,
        scratch_shapes=[pltpu.VMEM((2, 8192, 128), jnp.float32), pltpu.SemaphoreType.DMA((8,))],
        compiler_params=pltpu.CompilerParams(vmem_limit_bytes=40 * 2**20),
        name="pack",
    )(place, matrix, factor)


def iotas():
    return (
        lax.broadcasted_iota(jnp.int32, (NB, NB), 0),
        lax.broadcasted_iota(jnp.int32, (NB, NB), 1),
    )


def inverses(lowers, rows, cols):
    eye = rows == cols
    pair = (rows // 2 == cols // 2) & (rows > cols)
    first = []
    for lower in lowers:
        down = 1.0 / jnp.sum(jnp.where(eye, lower, 0.0), axis=1, keepdims=True)
        across = 1.0 / jnp.sum(jnp.where(eye, lower, 0.0), axis=0, keepdims=True)
        first.append(jnp.where(eye, down, 0.0) - jnp.where(pair, lower * down * across, 0.0))

    def double(level, values):
        size = jnp.right_shift(rows, level) - jnp.right_shift(cols, level)
        band = (size == 1) & (jnp.right_shift(rows, level + 1) == jnp.right_shift(cols, level + 1))
        blocks = [full(value, jnp.where(band, lower, 0.0), NN) for value, lower in zip(values, lowers)]
        return tuple(value - full(block, value, NN) for value, block in zip(values, blocks))

    return lax.fori_loop(1, 8, double, tuple(first))


def head_kernel(place, *rest):
    parts, (v0, s0, v1, s1, h0, l10, head) = rest[:9], rest[9:]
    z = place[2]
    for offset, part in zip((0, -1, 1, -2, 2, -3, 3), parts):
        head[(z + offset + SLABS) % SLABS] = part[...]
    far = (z + 4) % SLABS
    head[far, :6] = parts[7][...]
    head[far, 6:] = parts[8][...]
    rows, cols = iotas()
    eye = rows == cols

    def tile(k):
        return jnp.concatenate([head[:, 2 * k + half].reshape(NB, 128) for half in range(2)], axis=1)

    a00, l00, a10, low, a11, l11 = (tile(k) for k in range(6))
    inv0, inv1 = inverses((l00, l11), rows, cols)
    part = full(full(inv0, jnp.where(eye, 0.5 * a00, a00), NN), inv0)
    core0 = part + part.T
    half0 = full(a10, inv0) - 0.5 * full(low, core0)
    inner = jnp.where(eye, 0.5 * a11, a11) - full(half0, low)
    part = full(full(inv1, inner, NN), inv1)
    core1 = part + part.T
    v0[...] = inv0
    s0[...] = core0
    v1[...] = inv1
    s1[...] = core1
    h0[...] = half0
    l10[...] = low


def head_math(place, parts):
    parts = [part.reshape(-1, SLAB, 128) for part in parts]
    return pl.pallas_call(
        head_kernel,
        in_specs=[pl.BlockSpec(memory_space=pltpu.SMEM)] + [pl.BlockSpec(memory_space=pltpu.VMEM)] * 9,
        out_specs=[pl.BlockSpec(memory_space=pltpu.VMEM)] * 6,
        out_shape=[jax.ShapeDtypeStruct((NB, NB), jnp.float32)] * 6,
        scratch_shapes=[pltpu.VMEM((SLABS, 12, SLAB, 128), jnp.float32)],
        compiler_params=pltpu.CompilerParams(vmem_limit_bytes=16 * 2**20),
        name="head",
    )(place, *parts)


def main_kernel(place, raw_row, *rest):
    grids, (v0, s0, v1, s1, h0, l10, local, out, raw_col, col_hi, col_lo, head_hi, head_lo) = rest[:10], rest[10:]
    step = pl.program_id(0)
    p = place[0]
    c = place[1]

    def read(raw, core, m, tile):
        return jnp.concatenate([raw[:, core, m, tile, half].reshape(NB, 128) for half in range(2)], axis=1)

    def panels(raw, tile):
        def head(k):
            return head_hi[k], head_lo[k]

        a0, a1 = read(raw, 0, 0, tile), read(raw, 1, 0, tile)
        f0, f1 = split(read(raw, 0, 1, tile)), split(read(raw, 1, 1, tile))
        p0 = three(f0, head(1))
        half0 = three(split(a0), head(0)) - 0.5 * p0
        g0 = split(half0)
        a1 = a1 - three(g0, head(5)) - three(f0, head(4))
        p1 = three(f1, head(3))
        half1 = three(split(a1), head(2)) - 0.5 * p1
        g1 = split(half1)
        return g0, f0, g1, f1, half0 - 0.5 * p0, half1 - 0.5 * p1

    @pl.when(step == 0)
    def _():
        for k, ref in enumerate((v0, s0, v1, s1, h0, l10)):
            head_hi[k], head_lo[k] = split(ref[...])
        y, x = p // 4, p % 4

        def spot(dy, dx):
            return ((y + dy) % 4) * 4 + (x + dx) % 4

        for m in range(2):
            near, back, ahead, far_one, far_two = grids[5 * m : 5 * m + 5]
            order = (0, 3, 1, 2)
            for k in range(4):
                for part, dy in ((near, 0), (back, 3), (ahead, 1), (far_one if k < 2 else far_two, 2)):
                    dx = order[k]
                    at = spot(dy, dx) if m == 0 else spot(dx, dy)
                    index = k % 2 if dy == 2 else k
                    raw_col[at // 2, at % 2, m] = part[index]

        def one(tile, carry):
            g0, f0, g1, f1, _, _ = panels(raw_col, tile)
            for k, (hi, lo) in enumerate((f0, g0, f1, g1)):
                col_hi[tile, :, k * NB : (k + 1) * NB] = hi
                col_lo[tile, :, k * NB : (k + 1) * NB] = lo
            return carry

        lax.fori_loop(0, 4, one, 0)

    g0, f0, g1, f1, done0, done1 = panels(raw_row, step)
    row_hi = jnp.concatenate([g0[0], f0[0], g1[0], f1[0]], axis=1)
    row_lo = jnp.concatenate([g0[1], f0[1], g1[1], f1[1]], axis=1)
    rows, cols = iotas()

    def put(tile, value):
        for half in range(2):
            out[pl.ds(tile * 2 + half, NB, stride=8), :] = value[:, half * 128 : (half + 1) * 128]

    def get(tile):
        return jnp.concatenate([local[pl.ds(tile * 2 + half, NB, stride=8), :] for half in range(2)], axis=1)

    def update(tile, carry):
        below = (step > tile) | ((step == tile) & (p > c))
        same = (step == tile) & (p == c)
        ours = (below | same) & ((tile > 0) | (c > 1))

        @pl.when(ours)
        def _():
            change = three((row_hi, row_lo), (col_hi[tile], col_lo[tile]))
            keep = jnp.logical_or(below, rows >= cols)
            put(tile, get(tile) - jnp.where(keep, change, 0.0))

        @pl.when(jnp.logical_not(ours))
        def _():
            put(tile, get(tile))

        return carry

    lax.fori_loop(0, 4, update, 0)
    top = step * 16 + p
    for block, (done, core) in enumerate(((done0, s0), (done1, s1))):

        @pl.when((c == block) & (top > block))
        def _():
            put(0, done)

        @pl.when((c == block) & (top == block))
        def _():
            put(0, jnp.where(rows >= cols, core[...], 0.0))


def main_math(place, raw_row, grids, head, local):
    def whole(shape):
        return pl.BlockSpec(shape, lambda i: (0,) * len(shape))

    raw = (SLABS, 2, 2, 4, 2, SLAB, 128)
    block = pl.BlockSpec((2048, 128), lambda i: (i, 0))
    vmem = pl.BlockSpec(memory_space=pltpu.VMEM)
    grids = [part.reshape(-1, 4, 2, SLAB, 128) for part in grids]
    return pl.pallas_call(
        main_kernel,
        grid=(4,),
        in_specs=[pl.BlockSpec(memory_space=pltpu.SMEM), whole(raw)] + [vmem] * 16 + [block],
        out_specs=block,
        out_shape=jax.ShapeDtypeStruct((8192, 128), jnp.float32),
        scratch_shapes=[
            pltpu.VMEM(raw, jnp.float32),
            pltpu.VMEM((4, NB, 4 * NB), jnp.bfloat16),
            pltpu.VMEM((4, NB, 4 * NB), jnp.bfloat16),
            pltpu.VMEM((6, NB, NB), jnp.bfloat16),
            pltpu.VMEM((6, NB, NB), jnp.bfloat16),
        ],
        compiler_params=pltpu.CompilerParams(vmem_limit_bytes=36 * 2**20),
        name="main",
    )(place, raw_row.reshape(raw), *grids, *head, local)


def shift(value, axis, size, by):
    return lax.ppermute(value, axis, [(i, (i + by) % size) for i in range(size)])


def ring8(value):
    up1, down1 = shift(value, "z", 8, 1), shift(value, "z", 8, -1)
    up2, down2 = shift(up1, "z", 8, 1), shift(down1, "z", 8, -1)
    up3, down3 = shift(up2, "z", 8, 1), shift(down2, "z", 8, -1)
    half = value.shape[0] // 2
    up4, down4 = shift(up3[:half], "z", 8, 1), shift(down3[half:], "z", 8, -1)
    return [value, up1, down1, up2, down2, up3, down3, up4, down4]


def ring4(value, axis):
    up, down = shift(value, axis, 4, 1), shift(value, axis, 4, -1)
    half = value.shape[0] // 2
    return [value, up, down, shift(up[:half], axis, 4, 1), shift(down[half:], axis, 4, -1)]


def on_device(matrix, factor):
    x, y, z, core = (lax.axis_index(name) for name in ("x", "y", "z", "core"))
    p = lax.axis_index(ROW)
    c = lax.axis_index(COL)
    place = jnp.stack([p, c, z])
    local = matrix.reshape(8192, 128)
    pieces = pack(place, local, factor.reshape(8192, 128))
    order = (4, 1, 7, 2, 6, 3, 5)
    got = [lax.ppermute(pieces[k], "z", [(0, k)]) for k in order]
    total = got[0]
    for value in got[1:]:
        total = total + value
    mine = jnp.where(z == 0, pieces[0], total)
    raw_row = lax.all_gather(mine, COL)

    swapped = lax.ppermute(mine, ROW + COL, [(r * 16 + j, j * 16 + r) for r in range(16) for j in range(16)])
    first = ring4(swapped[: 8 * SLAB], "x")
    second = ring4(swapped[8 * SLAB :], "y")
    grids = ring4(jnp.concatenate(first, 0), "y") + ring4(jnp.concatenate(second, 0), "x")

    top = mine.reshape(2, 4, 2 * SLAB, 128)[:, 0].reshape(4 * SLAB, 128)
    other = lax.ppermute(top, "core", [(0, 1), (1, 0)])
    both = jnp.where(core == 0, jnp.concatenate([top, other], 0), jnp.concatenate([other, top], 0))
    across = lax.ppermute(both, ROW, [(0, 1), (1, 0)])
    zero, one = jnp.where(p == 0, both, across), jnp.where(p == 0, across, both)
    head = jnp.concatenate([zero[: 4 * SLAB], one], 0)
    sent = lax.ppermute(head, ROW, [(0, 3), (1, 2)])
    head = jnp.where(x < 2, head, sent)
    sent1 = lax.ppermute(head, "y", [(0, 1)])
    sent3 = lax.ppermute(head, "y", [(0, 3)])
    sent2 = lax.ppermute(sent1, "y", [(1, 2)])
    head = jnp.where(y == 0, head, jnp.where(y == 1, sent1, jnp.where(y == 2, sent2, sent3)))
    head = head_math(place, ring8(head))
    return main_math(place, raw_row, grids, head, local).reshape(matrix.shape)


def solution(mesh):
    torus = Mesh(mesh.devices.reshape(4, 4, 8, 2), ("y", "x", "z", "core"))
    spec = P(None, ROW, None, None, COL, None)
    return jax.shard_map(on_device, mesh=torus, in_specs=(spec, spec), out_specs=spec, check_vma=False)
```

```python
import jax
import jax.numpy as jnp
from jax import lax
from jax.experimental import pallas as pl
from jax.experimental.pallas import tpu as pltpu
from jax.sharding import Mesh
from jax.sharding import PartitionSpec as P


NB = 256
ROW = ("y", "x")
COL = ("z", "core")
SLABS = 8
SLAB = NB // SLABS


NT = (((1,), (1,)), ((), ()))
NN = (((1,), (0,)), ((), ()))


def full(left, right, dims=NT):
    return lax.dot_general(left, right, dims, precision=lax.Precision.HIGHEST, preferred_element_type=jnp.float32)


def split(value):
    high = value.astype(jnp.bfloat16)
    return high, (value - high.astype(jnp.float32)).astype(jnp.bfloat16)


def three(left, right):
    def dot(a, b):
        return lax.dot_general(a, b, NT, preferred_element_type=jnp.float32)

    return dot(left[0], right[0]) + dot(left[0], right[1]) + dot(left[1], right[0])


def pack_kernel(place, matrix, factor, *rest):
    pieces, (buffer, sems) = rest[:SLABS], rest[SLABS:]

    @pl.when(place[2] == 0)
    def _():
        copies = {}
        for tile in range(4):
            for m, source in enumerate((matrix, factor)):
                rows = pl.ds(tile * 8 * NB, 8 * NB)
                copies[tile, m] = pltpu.make_async_copy(source.at[rows], buffer.at[m, rows], sems.at[m * 4 + tile])
                copies[tile, m].start()
        for tile in range(4):
            for m in range(2):
                copies[tile, m].wait()
                for half in range(2):
                    for slab in range(SLABS):
                        value = buffer[m, pl.ds((tile * NB + slab * SLAB) * 8 + half, SLAB, stride=8), :]
                        pieces[slab][pl.ds(((m * 4 + tile) * 2 + half) * SLAB, SLAB), :] = value


def pack(place, matrix, factor):
    return pl.pallas_call(
        pack_kernel,
        in_specs=[pl.BlockSpec(memory_space=pltpu.SMEM)] + [pl.BlockSpec(memory_space=pl.ANY)] * 2,
        out_specs=[pl.BlockSpec(memory_space=pltpu.VMEM)] * SLABS,
        out_shape=[jax.ShapeDtypeStruct((16 * SLAB, 128), jnp.float32)] * SLABS,
        scratch_shapes=[pltpu.VMEM((2, 8192, 128), jnp.float32), pltpu.SemaphoreType.DMA((8,))],
        compiler_params=pltpu.CompilerParams(vmem_limit_bytes=40 * 2**20),
        name="pack",
    )(place, matrix, factor)


def iotas():
    return (
        lax.broadcasted_iota(jnp.int32, (NB, NB), 0),
        lax.broadcasted_iota(jnp.int32, (NB, NB), 1),
    )


def inverses(lowers, rows, cols):
    eye = rows == cols
    pair = (rows // 2 == cols // 2) & (rows > cols)
    first = []
    for lower in lowers:
        down = 1.0 / jnp.sum(jnp.where(eye, lower, 0.0), axis=1, keepdims=True)
        across = 1.0 / jnp.sum(jnp.where(eye, lower, 0.0), axis=0, keepdims=True)
        first.append(jnp.where(eye, down, 0.0) - jnp.where(pair, lower * down * across, 0.0))

    def double(level, values):
        size = jnp.right_shift(rows, level) - jnp.right_shift(cols, level)
        band = (size == 1) & (jnp.right_shift(rows, level + 1) == jnp.right_shift(cols, level + 1))
        blocks = [full(value, jnp.where(band, lower, 0.0), NN) for value, lower in zip(values, lowers)]
        return tuple(value - full(block, value, NN) for value, block in zip(values, blocks))

    return lax.fori_loop(1, 8, double, tuple(first))


def head_kernel(place, *rest):
    parts, (out, head, done, sems) = rest[:9], rest[9:]
    z = place[2]
    for offset, part in zip((0, -1, 1, -2, 2, -3, 3), parts):
        head[(z + offset + SLABS) % SLABS] = part[...]
    far = (z + 4) % SLABS
    head[far, :6] = parts[7][...]
    head[far, 6:] = parts[8][...]
    rows, cols = iotas()
    eye = rows == cols

    def tile(k):
        return jnp.concatenate([head[:, 2 * k + half].reshape(NB, 128) for half in range(2)], axis=1)

    a00, l00, a10, low, a11, l11 = (tile(k) for k in range(6))
    inv0, inv1 = inverses((l00, l11), rows, cols)
    part = full(full(inv0, jnp.where(eye, 0.5 * a00, a00), NN), inv0)
    core0 = part + part.T
    half0 = full(a10, inv0) - 0.5 * full(low, core0)
    inner = jnp.where(eye, 0.5 * a11, a11) - full(half0, low)
    part = full(full(inv1, inner, NN), inv1)
    core1 = part + part.T
    copies = []
    for k, value in enumerate((inv0, core0, inv1, core1, half0, low)):
        done[k] = value
        copies.append(pltpu.make_async_copy(done.at[k], out.at[k], sems.at[k]))
        copies[k].start()
    for copy in copies:
        copy.wait()


def head_math(place, parts):
    parts = [part.reshape(-1, SLAB, 128) for part in parts]
    return pl.pallas_call(
        head_kernel,
        in_specs=[pl.BlockSpec(memory_space=pltpu.SMEM)] + [pl.BlockSpec(memory_space=pltpu.VMEM)] * 9,
        out_specs=pl.BlockSpec(memory_space=pltpu.HBM),
        out_shape=pltpu.HBM((6, NB, NB), jnp.float32),
        scratch_shapes=[
            pltpu.VMEM((SLABS, 12, SLAB, 128), jnp.float32),
            pltpu.VMEM((6, NB, NB), jnp.float32),
            pltpu.SemaphoreType.DMA((6,)),
        ],
        compiler_params=pltpu.CompilerParams(vmem_limit_bytes=16 * 2**20),
        name="head",
    )(place, *parts)


def main_kernel(place, raw_far, local_far, head_far, *rest):
    rows_in, rest = rest[:14], rest[14:]
    out, raw_row, raw_col, local, head, col_hi, col_lo, head_hi, head_lo, sems = rest
    step = pl.program_id(0)
    p = place[0]
    c = place[1]
    z = place[2]
    core = c % 2

    def load_local(tile):
        return pltpu.make_async_copy(local_far.at[pl.ds(tile * 2048, 2048)], local.at[tile], sems.at[tile])

    def read(raw, core, m, tile):
        return jnp.concatenate([raw[:, core, m, tile, half].reshape(NB, 128) for half in range(2)], axis=1)

    def panels(raw, tile):
        def heads(k):
            return head_hi[k], head_lo[k]

        a0, a1 = read(raw, 0, 0, tile), read(raw, 1, 0, tile)
        f0, f1 = split(read(raw, 0, 1, tile)), split(read(raw, 1, 1, tile))
        p0 = three(f0, heads(1))
        half0 = three(split(a0), heads(0)) - 0.5 * p0
        g0 = split(half0)
        a1 = a1 - three(g0, heads(5)) - three(f0, heads(4))
        p1 = three(f1, heads(3))
        half1 = three(split(a1), heads(2)) - 0.5 * p1
        g1 = split(half1)
        return g0, f0, g1, f1, half0 - 0.5 * p0, half1 - 0.5 * p1

    @pl.when(step == 0)
    def _():
        load_col = pltpu.make_async_copy(raw_far, raw_col, sems.at[4])
        load_head = pltpu.make_async_copy(head_far, head, sems.at[5])
        load_head.start()
        load_col.start()
        for tile in range(4):
            load_local(tile).start()
        for which, side in ((0, core), (1, 1 - core)):
            for k, offset in enumerate((0, -1, 1, -2, 2, -3, 3)):
                part = rows_in[k] if which == 0 else rows_in[9 + (k + 1) // 2]
                at = 0 if which == 0 or k == 0 else (k + 1) % 2
                raw_row[(z + offset + SLABS) % SLABS, side] = part[at]
            far = (z + 4) % SLABS
            for m in range(2):
                raw_row[far, side, m] = rows_in[7 + m][0] if which == 0 else rows_in[13][m]
        load_head.wait()
        for k in range(6):
            head_hi[k], head_lo[k] = split(head[k])
        load_col.wait()

        def one(tile, carry):
            g0, f0, g1, f1, _, _ = panels(raw_col, tile)
            for k, (hi, lo) in enumerate((f0, g0, f1, g1)):
                col_hi[tile, :, k * NB : (k + 1) * NB] = hi
                col_lo[tile, :, k * NB : (k + 1) * NB] = lo
            return carry

        lax.fori_loop(0, 4, one, 0)

    g0, f0, g1, f1, done0, done1 = panels(raw_row, step)
    load_local(step).wait()
    row_hi = jnp.concatenate([g0[0], f0[0], g1[0], f1[0]], axis=1)
    row_lo = jnp.concatenate([g0[1], f0[1], g1[1], f1[1]], axis=1)
    rows, cols = iotas()

    def put(tile, value):
        for half in range(2):
            out[pl.ds(tile * 2 + half, NB, stride=8), :] = value[:, half * 128 : (half + 1) * 128]

    def get(tile):
        return jnp.concatenate([local[step, pl.ds(tile * 2 + half, NB, stride=8), :] for half in range(2)], axis=1)

    def update(tile, carry):
        below = (step > tile) | ((step == tile) & (p > c))
        same = (step == tile) & (p == c)
        ours = (below | same) & ((tile > 0) | (c > 1))

        @pl.when(ours)
        def _():
            change = three((row_hi, row_lo), (col_hi[tile], col_lo[tile]))
            keep = jnp.logical_or(below, rows >= cols)
            put(tile, get(tile) - jnp.where(keep, change, 0.0))

        @pl.when(jnp.logical_not(ours))
        def _():
            put(tile, get(tile))

        return carry

    lax.fori_loop(0, 4, update, 0)
    top = step * 16 + p
    for block, done in enumerate((done0, done1)):

        @pl.when((c == block) & (top > block))
        def _():
            put(0, done)

        @pl.when((c == block) & (top == block))
        def _():
            put(0, jnp.where(rows >= cols, head[2 * block + 1], 0.0))


def main_math(place, rows, raw_col, head, local):
    raw = (SLABS, 2, 2, 4, 2, SLAB, 128)
    vmem = pl.BlockSpec(memory_space=pltpu.VMEM)
    hbm = pl.BlockSpec(memory_space=pltpu.HBM)
    whole = [rows[k].reshape(-1, 2, 4, 2, SLAB, 128) for k in (0, 1, 2, 3, 4, 5, 6)]
    halves = [rows[k].reshape(1, 4, 2, SLAB, 128) for k in (7, 8)]
    crossed = [rows[k].reshape(-1, 2, 4, 2, SLAB, 128) for k in (9, 10, 11, 12)] + [rows[13].reshape(2, 4, 2, SLAB, 128)]
    return pl.pallas_call(
        main_kernel,
        grid=(4,),
        in_specs=[pl.BlockSpec(memory_space=pltpu.SMEM), hbm, hbm, hbm] + [vmem] * 14,
        out_specs=pl.BlockSpec((2048, 128), lambda i: (i, 0)),
        out_shape=jax.ShapeDtypeStruct((8192, 128), jnp.float32),
        scratch_shapes=[
            pltpu.VMEM(raw, jnp.float32),
            pltpu.VMEM(raw, jnp.float32),
            pltpu.VMEM((4, 2048, 128), jnp.float32),
            pltpu.VMEM((6, NB, NB), jnp.float32),
            pltpu.VMEM((4, NB, 4 * NB), jnp.bfloat16),
            pltpu.VMEM((4, NB, 4 * NB), jnp.bfloat16),
            pltpu.VMEM((6, NB, NB), jnp.bfloat16),
            pltpu.VMEM((6, NB, NB), jnp.bfloat16),
            pltpu.SemaphoreType.DMA((6,)),
        ],
        compiler_params=pltpu.CompilerParams(vmem_limit_bytes=32 * 2**20),
        name="main",
    )(place, far(raw_col.reshape(raw)), far(local), far(head), *whole, *halves, *crossed)


def shift(value, axis, size, by):
    return lax.ppermute(value, axis, [(i, (i + by) % size) for i in range(size)])


def ring8(value):
    up1, down1 = shift(value, "z", 8, 1), shift(value, "z", 8, -1)
    up2, down2 = shift(up1, "z", 8, 1), shift(down1, "z", 8, -1)
    up3, down3 = shift(up2, "z", 8, 1), shift(down2, "z", 8, -1)
    half = value.shape[0] // 2
    up4, down4 = shift(up3[:half], "z", 8, 1), shift(down3[half:], "z", 8, -1)
    return [value, up1, down1, up2, down2, up3, down3, up4, down4]


def far(value):
    return pltpu.with_memory_space_constraint(value, pltpu.HBM)


def crossed(*values):
    return lax.ppermute(jnp.concatenate(values, 0), "core", [(0, 1), (1, 0)])


def device(matrix, factor):
    x, y, z, core = (lax.axis_index(name) for name in ("x", "y", "z", "core"))
    p = lax.axis_index(ROW)
    c = lax.axis_index(COL)
    place = jnp.stack([p, c, z])
    local = matrix.reshape(8192, 128)
    pieces = pack(place, local, factor.reshape(8192, 128))
    order = (4, 1, 7, 2, 6, 3, 5)
    got = [lax.ppermute(pieces[k], "z", [(0, k)]) for k in order]
    total = got[0]
    for value in got[1:]:
        total = total + value
    mine = jnp.where(z == 0, pieces[0], total)
    swapped = lax.ppermute(mine, ROW + COL, [(r * 16 + j, j * 16 + r) for r in range(16) for j in range(16)])
    top = mine.reshape(2, 4, 2 * SLAB, 128)[:, 0].reshape(4 * SLAB, 128)
    other = lax.ppermute(top, "core", [(0, 1), (1, 0)])
    both = jnp.where(core == 0, jnp.concatenate([top, other], 0), jnp.concatenate([other, top], 0))
    across = lax.ppermute(both, ROW, [(0, 1), (1, 0)])
    zero, one = jnp.where(p == 0, both, across), jnp.where(p == 0, across, both)
    head = jnp.concatenate([zero[: 4 * SLAB], one], 0)
    sent = lax.ppermute(head, ROW, [(0, 3), (1, 2)])
    head = jnp.where(x < 2, head, sent)
    sent1 = lax.ppermute(head, "y", [(0, 1)])
    sent3 = lax.ppermute(head, "y", [(0, 3)])
    swapped, sent1, sent3 = lax.optimization_barrier((swapped, sent1, sent3))
    raw_col = lax.all_gather(swapped, ROW)
    sent2 = lax.ppermute(sent1, "y", [(1, 2)])
    head = jnp.where(y == 0, head, jnp.where(y == 1, sent1, jnp.where(y == 2, sent2, sent3)))
    head = head_math(place, ring8(head))
    rows = ring8(mine)
    rows = rows + [crossed(*rows[k : k + 2]) if k else crossed(rows[0]) for k in (0, 1, 3, 5, 7)]
    return main_math(place, rows, raw_col, head, local).reshape(matrix.shape)


def solution(mesh):
    torus = Mesh(mesh.devices.reshape(4, 4, 8, 2), ("y", "x", "z", "core"))
    spec = P(None, ROW, None, None, COL, None)
    return jax.shard_map(device, mesh=torus, in_specs=(spec, spec), out_specs=spec, check_vma=False)
```

```python
import jax
import jax.numpy as jnp
from jax import lax
from jax.experimental import pallas as pl
from jax.experimental.pallas import tpu as pltpu
from jax.sharding import Mesh
from jax.sharding import PartitionSpec as P


NB = 256
ROW = ("y", "x")
COL = ("z", "core")
SLABS = 8
SLAB = NB // SLABS


NT = (((1,), (1,)), ((), ()))
NN = (((1,), (0,)), ((), ()))


def full(left, right, dims=NT):
    return lax.dot_general(left, right, dims, precision=lax.Precision.HIGHEST, preferred_element_type=jnp.float32)


def split(value):
    high = value.astype(jnp.bfloat16)
    return high, (value - high.astype(jnp.float32)).astype(jnp.bfloat16)


def three(left, right):
    def dot(a, b):
        return lax.dot_general(a, b, NT, preferred_element_type=jnp.float32)

    return dot(left[0], right[0]) + dot(left[0], right[1]) + dot(left[1], right[0])


def pack_kernel(place, matrix, factor, *rest):
    pieces, (buffer, sems) = rest[:SLABS], rest[SLABS:]

    @pl.when(place[2] == 0)
    def _():
        copies = {}
        for tile in range(4):
            for m, source in enumerate((matrix, factor)):
                rows = pl.ds(tile * 8 * NB, 8 * NB)
                copies[tile, m] = pltpu.make_async_copy(source.at[rows], buffer.at[m, rows], sems.at[m * 4 + tile])
                copies[tile, m].start()
        for tile in range(4):
            for m in range(2):
                copies[tile, m].wait()
                for half in range(2):
                    for slab in range(SLABS):
                        value = buffer[m, pl.ds((tile * NB + slab * SLAB) * 8 + half, SLAB, stride=8), :]
                        pieces[slab][pl.ds(((m * 4 + tile) * 2 + half) * SLAB, SLAB), :] = value


def pack(place, matrix, factor):
    return pl.pallas_call(
        pack_kernel,
        in_specs=[pl.BlockSpec(memory_space=pltpu.SMEM)] + [pl.BlockSpec(memory_space=pl.ANY)] * 2,
        out_specs=[pl.BlockSpec(memory_space=pltpu.VMEM)] * SLABS,
        out_shape=[jax.ShapeDtypeStruct((16 * SLAB, 128), jnp.float32)] * SLABS,
        scratch_shapes=[pltpu.VMEM((2, 8192, 128), jnp.float32), pltpu.SemaphoreType.DMA((8,))],
        compiler_params=pltpu.CompilerParams(vmem_limit_bytes=40 * 2**20),
        name="pack",
    )(place, matrix, factor)


def iotas():
    return (
        lax.broadcasted_iota(jnp.int32, (NB, NB), 0),
        lax.broadcasted_iota(jnp.int32, (NB, NB), 1),
    )


def inverses(lowers, rows, cols):
    eye = rows == cols
    pair = (rows // 2 == cols // 2) & (rows > cols)
    first = []
    for lower in lowers:
        down = 1.0 / jnp.sum(jnp.where(eye, lower, 0.0), axis=1, keepdims=True)
        across = 1.0 / jnp.sum(jnp.where(eye, lower, 0.0), axis=0, keepdims=True)
        first.append(jnp.where(eye, down, 0.0) - jnp.where(pair, lower * down * across, 0.0))

    def double(level, values):
        size = jnp.right_shift(rows, level) - jnp.right_shift(cols, level)
        band = (size == 1) & (jnp.right_shift(rows, level + 1) == jnp.right_shift(cols, level + 1))
        blocks = [full(value, jnp.where(band, lower, 0.0), NN) for value, lower in zip(values, lowers)]
        return tuple(value - full(block, value, NN) for value, block in zip(values, blocks))

    return lax.fori_loop(1, 8, double, tuple(first))


def head_kernel(parts, out, head, done, sems):
    load = pltpu.make_async_copy(parts, head, sems.at[6])
    load.start()
    load.wait()
    rows, cols = iotas()
    eye = rows == cols

    def tile(k):
        return jnp.concatenate([head[:, k // 3, 2 * (k % 3) + half].reshape(NB, 128) for half in range(2)], axis=1)

    a00, l00, a10, low, a11, l11 = (tile(k) for k in range(6))
    inv0, inv1 = inverses((l00, l11), rows, cols)
    part = full(full(inv0, jnp.where(eye, 0.5 * a00, a00), NN), inv0)
    core0 = part + part.T
    half0 = full(a10, inv0) - 0.5 * full(low, core0)
    inner = jnp.where(eye, 0.5 * a11, a11) - full(half0, low)
    part = full(full(inv1, inner, NN), inv1)
    core1 = part + part.T
    copies = []
    for k, value in enumerate((inv0, core0, inv1, core1, half0, low)):
        done[k] = value
        copies.append(pltpu.make_async_copy(done.at[k], out.at[k], sems.at[k]))
        copies[k].start()
    for copy in copies:
        copy.wait()


def head_math(parts):
    shape = (SLABS, 2, 6, SLAB, 128)
    return pl.pallas_call(
        head_kernel,
        in_specs=[pl.BlockSpec(memory_space=pltpu.HBM)],
        out_specs=pl.BlockSpec(memory_space=pltpu.HBM),
        out_shape=pltpu.HBM((6, NB, NB), jnp.float32),
        scratch_shapes=[
            pltpu.VMEM(shape, jnp.float32),
            pltpu.VMEM((6, NB, NB), jnp.float32),
            pltpu.SemaphoreType.DMA((7,)),
        ],
        compiler_params=pltpu.CompilerParams(vmem_limit_bytes=16 * 2**20),
        name="head",
    )(far(parts.reshape(shape)))


def main_kernel(place, raw_far, local_far, head_far, *rest):
    grids, rest = rest[:10], rest[10:]
    out, raw_row, raw_col, local, head, col_hi, col_lo, head_hi, head_lo, sems = rest
    step = pl.program_id(0)
    p = place[0]
    c = place[1]

    def load_local(tile):
        return pltpu.make_async_copy(local_far.at[pl.ds(tile * 2048, 2048)], local.at[tile], sems.at[tile])

    def read(raw, core, m, tile):
        return jnp.concatenate([raw[:, core, m, tile, half].reshape(NB, 128) for half in range(2)], axis=1)

    def panels(raw, tile):
        def heads(k):
            return head_hi[k], head_lo[k]

        a0, a1 = read(raw, 0, 0, tile), read(raw, 1, 0, tile)
        f0, f1 = split(read(raw, 0, 1, tile)), split(read(raw, 1, 1, tile))
        p0 = three(f0, heads(1))
        half0 = three(split(a0), heads(0)) - 0.5 * p0
        g0 = split(half0)
        a1 = a1 - three(g0, heads(5)) - three(f0, heads(4))
        p1 = three(f1, heads(3))
        half1 = three(split(a1), heads(2)) - 0.5 * p1
        g1 = split(half1)
        return g0, f0, g1, f1, half0 - 0.5 * p0, half1 - 0.5 * p1

    @pl.when(step == 0)
    def _():
        load_row = pltpu.make_async_copy(raw_far, raw_row, sems.at[4])
        load_head = pltpu.make_async_copy(head_far, head, sems.at[5])
        load_head.start()
        load_row.start()
        for tile in range(4):
            load_local(tile).start()
        y, x = p // 4, p % 4

        def spot(dy, dx):
            return (((y + dy) % 4) * 4 + (x + dx) % 4 + 16 - c) % 16

        for m in range(2):
            near, back, ahead, far_one, far_two = grids[5 * m : 5 * m + 5]
            order = (0, 3, 1, 2)
            for k in range(4):
                for part, dy in ((near, 0), (back, 3), (ahead, 1), (far_one if k < 2 else far_two, 2)):
                    dx = order[k]
                    at = spot(dy, dx) if m == 0 else spot(dx, dy)
                    index = k % 2 if dy == 2 else k
                    raw_col[at // 2, at % 2, m] = part[index]
        load_head.wait()
        for k in range(6):
            head_hi[k], head_lo[k] = split(head[k])

        def one(tile, carry):
            g0, f0, g1, f1, _, _ = panels(raw_col, tile)
            for k, (hi, lo) in enumerate((f0, g0, f1, g1)):
                col_hi[tile, :, k * NB : (k + 1) * NB] = hi
                col_lo[tile, :, k * NB : (k + 1) * NB] = lo
            return carry

        lax.fori_loop(0, 4, one, 0)
        load_row.wait()

    g0, f0, g1, f1, done0, done1 = panels(raw_row, step)
    load_local(step).wait()
    row_hi = jnp.concatenate([g0[0], f0[0], g1[0], f1[0]], axis=1)
    row_lo = jnp.concatenate([g0[1], f0[1], g1[1], f1[1]], axis=1)
    rows, cols = iotas()

    def put(tile, value):
        for half in range(2):
            out[pl.ds(tile * 2 + half, NB, stride=8), :] = value[:, half * 128 : (half + 1) * 128]

    def get(tile):
        return jnp.concatenate([local[step, pl.ds(tile * 2 + half, NB, stride=8), :] for half in range(2)], axis=1)

    def update(tile, carry):
        below = (step > tile) | ((step == tile) & (p > c))
        same = (step == tile) & (p == c)
        ours = (below | same) & ((tile > 0) | (c > 1))

        @pl.when(ours)
        def _():
            change = three((row_hi, row_lo), (col_hi[tile], col_lo[tile]))
            keep = jnp.logical_or(below, rows >= cols)
            put(tile, get(tile) - jnp.where(keep, change, 0.0))

        @pl.when(jnp.logical_not(ours))
        def _():
            put(tile, get(tile))

        return carry

    lax.fori_loop(0, 4, update, 0)
    top = step * 16 + p
    for block, done in enumerate((done0, done1)):

        @pl.when((c == block) & (top > block))
        def _():
            put(0, done)

        @pl.when((c == block) & (top == block))
        def _():
            put(0, jnp.where(rows >= cols, head[2 * block + 1], 0.0))


def main_math(place, raw_row, grids, head, local):
    raw = (SLABS, 2, 2, 4, 2, SLAB, 128)
    vmem = pl.BlockSpec(memory_space=pltpu.VMEM)
    hbm = pl.BlockSpec(memory_space=pltpu.HBM)
    grids = [part.reshape(-1, 4, 2, SLAB, 128) for part in grids]
    return pl.pallas_call(
        main_kernel,
        grid=(4,),
        in_specs=[pl.BlockSpec(memory_space=pltpu.SMEM), hbm, hbm, hbm] + [vmem] * 10,
        out_specs=pl.BlockSpec((2048, 128), lambda i: (i, 0)),
        out_shape=jax.ShapeDtypeStruct((8192, 128), jnp.float32),
        scratch_shapes=[
            pltpu.VMEM(raw, jnp.float32),
            pltpu.VMEM(raw, jnp.float32),
            pltpu.VMEM((4, 2048, 128), jnp.float32),
            pltpu.VMEM((6, NB, NB), jnp.float32),
            pltpu.VMEM((4, NB, 4 * NB), jnp.bfloat16),
            pltpu.VMEM((4, NB, 4 * NB), jnp.bfloat16),
            pltpu.VMEM((6, NB, NB), jnp.bfloat16),
            pltpu.VMEM((6, NB, NB), jnp.bfloat16),
            pltpu.SemaphoreType.DMA((6,)),
        ],
        compiler_params=pltpu.CompilerParams(vmem_limit_bytes=32 * 2**20),
        name="main",
    )(place, far(raw_row.reshape(raw)), far(local), far(head), *grids)


def shift(value, axis, size, by):
    return lax.ppermute(value, axis, [(i, (i + by) % size) for i in range(size)])


def far(value):
    return pltpu.with_memory_space_constraint(value, pltpu.HBM)


def ring4(value, axis):
    up, down = shift(value, axis, 4, 1), shift(value, axis, 4, -1)
    half = value.shape[0] // 2
    return [value, up, down, shift(up[:half], axis, 4, 1), shift(down[half:], axis, 4, -1)]


def device(matrix, factor):
    x, y, z, core = (lax.axis_index(name) for name in ("x", "y", "z", "core"))
    p = lax.axis_index(ROW)
    c = lax.axis_index(COL)
    place = jnp.stack([p, c, z])
    local = matrix.reshape(8192, 128)
    pieces = pack(place, local, factor.reshape(8192, 128))
    order = (4, 1, 7, 2, 6, 3, 5)
    got = [lax.ppermute(pieces[k], "z", [(0, k)]) for k in order]
    total = got[0]
    for value in got[1:]:
        total = total + value
    mine = jnp.where(z == 0, pieces[0], total)
    raw_row = lax.all_gather(mine, COL)

    moved = lax.ppermute(mine, ROW + COL, [(r * 16 + j, (j + r) % 16 * 16 + j) for r in range(16) for j in range(16)])
    swapped = lax.ppermute(moved, ROW + COL, [(q * 16 + j, q * 16 + (q - j) % 16) for q in range(16) for j in range(16)])

    top = mine.reshape(2, 4, 2 * SLAB, 128)[:, 0].reshape(4 * SLAB, 128)
    other = lax.ppermute(top, "core", [(0, 1), (1, 0)])
    both = jnp.where(core == 0, jnp.concatenate([top, other], 0), jnp.concatenate([other, top], 0))
    across = lax.ppermute(both, ROW, [(0, 1), (1, 0)])
    zero, one = jnp.where(p == 0, both, across), jnp.where(p == 0, across, both)
    head = jnp.concatenate([zero[: 4 * SLAB], one], 0)
    sent = lax.ppermute(head, ROW, [(0, 3), (1, 2)])
    head = jnp.where(x < 2, head, sent)
    sent1 = lax.ppermute(head, "y", [(0, 1)])
    sent3 = lax.ppermute(head, "y", [(0, 3)])
    sent2 = lax.ppermute(sent1, "y", [(1, 2)])
    head = jnp.where(y == 0, head, jnp.where(y == 1, sent1, jnp.where(y == 2, sent2, sent3)))
    half = jnp.where(core == 0, head[: 6 * SLAB], head[6 * SLAB :])
    half = lax.all_gather(half, COL)
    head = head_math(half)

    first = ring4(swapped[: 8 * SLAB], "x")
    second = ring4(swapped[8 * SLAB :], "y")
    grids = ring4(jnp.concatenate(first, 0), "y") + ring4(jnp.concatenate(second, 0), "x")
    return main_math(place, raw_row, grids, head, local).reshape(matrix.shape)


def solution(mesh):
    torus = Mesh(mesh.devices.reshape(4, 4, 8, 2), ("y", "x", "z", "core"))
    spec = P(None, ROW, None, None, COL, None)
    return jax.shard_map(device, mesh=torus, in_specs=(spec, spec), out_specs=spec, check_vma=False)
```

```python
import jax
import jax.numpy as jnp
from jax import lax
from jax.experimental import pallas as pl
from jax.experimental.pallas import tpu as pltpu
from jax.sharding import Mesh
from jax.sharding import PartitionSpec as P


NB = 256
ROW = ("y", "x")
COL = ("z", "core")
SLABS = 8
SLAB = NB // SLABS


NT = (((1,), (1,)), ((), ()))
NN = (((1,), (0,)), ((), ()))


def full(left, right, dims=NT):
    return lax.dot_general(left, right, dims, precision=lax.Precision.HIGHEST, preferred_element_type=jnp.float32)


def split(value):
    high = value.astype(jnp.bfloat16)
    return high, (value - high.astype(jnp.float32)).astype(jnp.bfloat16)


def three(left, right, dims=NT):
    def dot(a, b):
        return lax.dot_general(a, b, dims, preferred_element_type=jnp.float32)

    return dot(left[0], right[0]) + dot(left[0], right[1]) + dot(left[1], right[0])


def quick(left, right, dims=NT):
    return three(split(left), split(right), dims)


def pack_kernel(place, matrix, factor, *rest):
    pieces, (buffer, sems) = rest[:SLABS], rest[SLABS:]

    @pl.when(place[2] == 0)
    def _():
        copies = {}
        for tile in range(4):
            for m, source in enumerate((matrix, factor)):
                rows = pl.ds(tile * 8 * NB, 8 * NB)
                copies[tile, m] = pltpu.make_async_copy(source.at[rows], buffer.at[m, rows], sems.at[m * 4 + tile])
                copies[tile, m].start()
        for tile in range(4):
            for m in range(2):
                copies[tile, m].wait()
                for half in range(2):
                    for slab in range(SLABS):
                        value = buffer[m, pl.ds((tile * NB + slab * SLAB) * 8 + half, SLAB, stride=8), :]
                        pieces[slab][pl.ds(((m * 4 + tile) * 2 + half) * SLAB, SLAB), :] = value


def pack(place, matrix, factor):
    return pl.pallas_call(
        pack_kernel,
        in_specs=[pl.BlockSpec(memory_space=pltpu.SMEM)] + [pl.BlockSpec(memory_space=pltpu.HBM)] * 2,
        out_specs=[pl.BlockSpec(memory_space=pltpu.VMEM)] * SLABS,
        out_shape=[jax.ShapeDtypeStruct((16 * SLAB, 128), jnp.float32)] * SLABS,
        scratch_shapes=[pltpu.VMEM((2, 8192, 128), jnp.float32), pltpu.SemaphoreType.DMA((8,))],
        compiler_params=pltpu.CompilerParams(vmem_limit_bytes=40 * 2**20),
        name="pack",
    )(place, far(matrix), far(factor))


def iotas():
    return (
        lax.broadcasted_iota(jnp.int32, (NB, NB), 0),
        lax.broadcasted_iota(jnp.int32, (NB, NB), 1),
    )


def inverses(lowers):
    half = NB // 2
    rows = lax.broadcasted_iota(jnp.int32, (half, NB), 0)
    cols = lax.broadcasted_iota(jnp.int32, (half, NB), 1) % half
    eye = rows == cols
    left = lax.broadcasted_iota(jnp.int32, (half, NB), 1) < half

    def spread(value):
        return jnp.concatenate([jnp.where(left, value, 0.0), jnp.where(left, 0.0, value)], axis=0)

    compact = [jnp.concatenate([lower[:half, :half], lower[half:, half:]], axis=1) for lower in lowers]
    first = []
    for value in compact:
        diagonal = jnp.where(eye, value, 0.0)
        across = 1.0 / jnp.sum(diagonal, axis=0, keepdims=True)
        down = [1.0 / jnp.sum(jnp.where(side, diagonal, 0.0), axis=1, keepdims=True) for side in (left, ~left)]
        down = jnp.where(left, down[0], down[1])
        pair = (rows // 2 == cols // 2) & (rows > cols)
        first.append(jnp.where(eye, across, 0.0) - jnp.where(pair, value * down * across, 0.0))

    def double(level, values):
        step = jnp.right_shift(rows, level) - jnp.right_shift(cols, level)
        band = (step == 1) & (jnp.right_shift(rows, level + 1) == jnp.right_shift(cols, level + 1))
        blocks = [quick(value, spread(jnp.where(band, whole, 0.0)), NN) for value, whole in zip(values, compact)]
        return tuple(value - quick(block, spread(value), NN) for value, block in zip(values, blocks))

    values = lax.fori_loop(1, 7, double, tuple(first))
    out = []
    for value, lower in zip(values, lowers):
        top, low = value[:, :half], value[:, half:]
        corner = quick(quick(low, lower[half:, :half], NN), top, NN)
        result = jnp.concatenate([jnp.where(left, value, 0.0), jnp.concatenate([-corner, low], axis=1)], axis=0)
        diag_rows, diag_cols = iotas()
        rest = jnp.where(diag_rows == diag_cols, 1.0, 0.0) - full(lower, result, NN)
        out.append(result + quick(result, rest, NN))
    return out


def head_math(tile, head_hi, head_lo, cores):
    a00, l00, a10, low, a11, l11 = (tile(*k) for k in ((0, 0, 0), (0, 0, 1), (0, 1, 0), (0, 1, 1), (1, 1, 0), (1, 1, 1)))
    rows, cols = iotas()
    eye = rows == cols

    def keep(k, value):
        head_hi[k], head_lo[k] = split(value)
        return head_hi[k], head_lo[k]

    inv0, inv1 = inverses((l00, l11))
    inv0, inv1, low = keep(0, inv0), keep(2, inv1), keep(5, low)
    part = three(split(three(inv0, split(jnp.where(eye, 0.5 * a00, a00)), NN)), inv0)
    cores[0] = part + part.T
    half0 = keep(4, three(split(a10), inv0) - 0.5 * three(low, keep(1, cores[0])))
    inner = jnp.where(eye, 0.5 * a11, a11) - three(half0, low)
    part = three(split(three(inv1, split(inner), NN)), inv1)
    cores[1] = part + part.T
    keep(3, cores[1])


def main_kernel(place, raw_far, local_far, *rest):
    grids, rest = rest[:10], rest[10:]
    out, raw_row, raw_col, local, head, cores, col_hi, col_lo, head_hi, head_lo, sems = rest
    step = pl.program_id(0)
    p = place[0]
    c = place[1]

    def load_local(tile):
        return pltpu.make_async_copy(local_far.at[pl.ds(tile * 2048, 2048)], local.at[tile], sems.at[tile])

    def read(raw, core, m, tile):
        at = (m * 4 + tile) * 2
        return jnp.concatenate([raw[:, core, at + half].reshape(NB, 128) for half in range(2)], axis=1)

    def panels(raw, tile):
        def heads(k):
            return head_hi[k], head_lo[k]

        a0, a1 = read(raw, 0, 0, tile), read(raw, 1, 0, tile)
        f0, f1 = split(read(raw, 0, 1, tile)), split(read(raw, 1, 1, tile))
        p0 = three(f0, heads(1))
        half0 = three(split(a0), heads(0)) - 0.5 * p0
        g0 = split(half0)
        a1 = a1 - three(g0, heads(5)) - three(f0, heads(4))
        p1 = three(f1, heads(3))
        half1 = three(split(a1), heads(2)) - 0.5 * p1
        g1 = split(half1)
        return g0, f0, g1, f1, half0 - 0.5 * p0, half1 - 0.5 * p1

    @pl.when(step == 0)
    def _():
        load_row = pltpu.make_async_copy(raw_far.at[:, :, pl.ds(0, 16)], raw_row, sems.at[4])
        load_head = pltpu.make_async_copy(raw_far.at[:, :, pl.ds(16, 8)], head, sems.at[5])
        load_head.start()
        load_row.start()
        for tile in range(4):
            load_local(tile).start()
        y, x = p // 4, p % 4
        loads = []

        def spot(dy, dx):
            return (((y + dy) % 4) * 4 + (x + dx) % 4 + 16 - c) % 16

        for m in range(2):
            near, back, ahead, far_one, far_two = grids[5 * m : 5 * m + 5]
            order = (0, 3, 1, 2)
            for k in range(4):
                for part, dy in ((near, 0), (back, 3), (ahead, 1), (far_one if k < 2 else far_two, 2)):
                    dx = order[k]
                    at = spot(dy, dx) if m == 0 else spot(dx, dy)
                    if dy == 2:
                        slot = raw_col.at[at // 2, at % 2, pl.ds(8 * m, 8)]
                        loads.append(pltpu.make_async_copy(part.at[k % 2], slot, sems.at[6 + 4 * m + k]))
                        loads[-1].start()
                    else:
                        raw_col[at // 2, at % 2, 8 * m : 8 * m + 8] = part[k]
        load_head.wait()

        def square(core, row, m):
            at = (row * 2 + m) * 2
            return jnp.concatenate([head[:, core, at + half].reshape(NB, 128) for half in range(2)], axis=1)

        head_math(square, head_hi, head_lo, cores)
        for load in loads:
            load.wait()

        def one(tile, carry):
            g0, f0, g1, f1, _, _ = panels(raw_col, tile)
            for k, (hi, lo) in enumerate((f0, g0, f1, g1)):
                col_hi[tile, :, k * NB : (k + 1) * NB] = hi
                col_lo[tile, :, k * NB : (k + 1) * NB] = lo
            return carry

        lax.fori_loop(0, 4, one, 0)
        load_row.wait()

    g0, f0, g1, f1, done0, done1 = panels(raw_row, step)
    load_local(step).wait()
    row_hi = jnp.concatenate([g0[0], f0[0], g1[0], f1[0]], axis=1)
    row_lo = jnp.concatenate([g0[1], f0[1], g1[1], f1[1]], axis=1)
    rows, cols = iotas()

    def put(tile, value):
        for half in range(2):
            out[pl.ds(tile * 2 + half, NB, stride=8), :] = value[:, half * 128 : (half + 1) * 128]

    def get(tile):
        return jnp.concatenate([local[step, pl.ds(tile * 2 + half, NB, stride=8), :] for half in range(2)], axis=1)

    def update(tile, carry):
        below = (step > tile) | ((step == tile) & (p > c))
        same = (step == tile) & (p == c)
        ours = (below | same) & ((tile > 0) | (c > 1))

        @pl.when(ours)
        def _():
            change = three((row_hi, row_lo), (col_hi[tile], col_lo[tile]))
            keep = jnp.logical_or(below, rows >= cols)
            put(tile, get(tile) - jnp.where(keep, change, 0.0))

        @pl.when(jnp.logical_not(ours))
        def _():
            put(tile, get(tile))

        return carry

    lax.fori_loop(0, 4, update, 0)
    top = step * 16 + p
    for block, done in enumerate((done0, done1)):

        @pl.when((c == block) & (top > block))
        def _():
            put(0, done)

        @pl.when((c == block) & (top == block))
        def _():
            put(0, jnp.where(rows >= cols, cores[block], 0.0))


def main_math(place, raw_row, grids, local):
    raw = (SLABS, 2, 16, SLAB, 128)
    vmem = pl.BlockSpec(memory_space=pltpu.VMEM)
    hbm = pl.BlockSpec(memory_space=pltpu.HBM)
    grids = [part.reshape(-1, 8, SLAB, 128) for part in grids]
    grids = [far(part) if k % 5 > 2 else part for k, part in enumerate(grids)]
    places = [hbm if k % 5 > 2 else vmem for k in range(10)]
    return pl.pallas_call(
        main_kernel,
        grid=(4,),
        in_specs=[pl.BlockSpec(memory_space=pltpu.SMEM), hbm, hbm] + places,
        out_specs=pl.BlockSpec((2048, 128), lambda i: (i, 0)),
        out_shape=jax.ShapeDtypeStruct((8192, 128), jnp.float32),
        scratch_shapes=[
            pltpu.VMEM(raw, jnp.float32),
            pltpu.VMEM(raw, jnp.float32),
            pltpu.VMEM((4, 2048, 128), jnp.float32),
            pltpu.VMEM((SLABS, 2, 8, SLAB, 128), jnp.float32),
            pltpu.VMEM((2, NB, NB), jnp.float32),
            pltpu.VMEM((4, NB, 4 * NB), jnp.bfloat16),
            pltpu.VMEM((4, NB, 4 * NB), jnp.bfloat16),
            pltpu.VMEM((6, NB, NB), jnp.bfloat16),
            pltpu.VMEM((6, NB, NB), jnp.bfloat16),
            pltpu.SemaphoreType.DMA((14,)),
        ],
        compiler_params=pltpu.CompilerParams(vmem_limit_bytes=32 * 2**20),
        name="main",
    )(place, far(raw_row.reshape(SLABS, 2, 24, SLAB, 128)), far(local), *grids)


def shift(value, axis, size, by):
    return lax.ppermute(value, axis, [(i, (i + by) % size) for i in range(size)])


def far(value):
    return pltpu.with_memory_space_constraint(value, pltpu.HBM)


def ring4(value, axis):
    up, down = shift(value, axis, 4, 1), shift(value, axis, 4, -1)
    half = value.shape[0] // 2
    return [value, up, down, shift(up[:half], axis, 4, 1), shift(down[half:], axis, 4, -1)]


def device(matrix, factor):
    x, y, z, _ = (lax.axis_index(name) for name in ("x", "y", "z", "core"))
    p = lax.axis_index(ROW)
    c = lax.axis_index(COL)
    place = jnp.stack([p, c, z])
    local = matrix.reshape(8192, 128)
    pieces = pack(place, local, factor.reshape(8192, 128))
    order = (4, 1, 7, 2, 6, 3, 5)
    got = [lax.ppermute(pieces[k], "z", [(0, k)]) for k in order]
    total = got[0]
    for value in got[1:]:
        total = total + value
    mine = jnp.where(z == 0, pieces[0], total)
    moved = lax.ppermute(mine, ROW + COL, [(r * 16 + j, (j + r) % 16 * 16 + j) for r in range(16) for j in range(16)])
    swapped = lax.ppermute(moved, ROW + COL, [(q * 16 + j, q * 16 + (q - j) % 16) for q in range(16) for j in range(16)])

    top = mine.reshape(2, 4, 2 * SLAB, 128)[:, 0].reshape(4 * SLAB, 128)
    across = lax.ppermute(top, ROW, [(0, 1), (1, 0)])
    tops = jnp.concatenate([jnp.where(p == 0, top, across), jnp.where(p == 0, across, top)], 0)
    sent = lax.ppermute(tops, ROW, [(0, 3), (1, 2)])
    tops = jnp.where(x < 2, tops, sent)
    sent = [lax.ppermute(tops, "y", [(0, k)]) for k in (2, 1, 3)]
    tops = jnp.where(y == 0, tops, sent[0] + sent[1] + sent[2])
    raw_row = lax.all_gather(jnp.concatenate([mine, tops], 0), COL)

    first = ring4(swapped[: 8 * SLAB], "x")
    second = ring4(swapped[8 * SLAB :], "y")
    grids = ring4(jnp.concatenate(first, 0), "y") + ring4(jnp.concatenate(second, 0), "x")
    return main_math(place, raw_row, grids, local).reshape(matrix.shape)


def solution(mesh):
    torus = Mesh(mesh.devices.reshape(4, 4, 8, 2), ("y", "x", "z", "core"))
    spec = P(None, ROW, None, None, COL, None)
    return jax.shard_map(device, mesh=torus, in_specs=(spec, spec), out_specs=spec, check_vma=False)
```

```python
import jax
import jax.numpy as jnp
from jax import lax
from jax.experimental import pallas as pl
from jax.experimental.pallas import tpu as pltpu
from jax.sharding import Mesh
from jax.sharding import PartitionSpec as P


NB = 256
ROW = ("y", "x")
COL = ("z", "core")
SLABS = 8
SLAB = NB // SLABS


NT = (((1,), (1,)), ((), ()))
NN = (((1,), (0,)), ((), ()))


def full(left, right, dims=NT):
    return lax.dot_general(left, right, dims, precision=lax.Precision.HIGHEST, preferred_element_type=jnp.float32)


def split(value):
    high = value.astype(jnp.bfloat16)
    return high, (value - high.astype(jnp.float32)).astype(jnp.bfloat16)


def three(left, right, dims=NT):
    axis = dims[0][1][0]
    lhs = jnp.concatenate([left[0], left[0], left[1]], axis=1)
    rhs = jnp.concatenate([right[0], right[1], right[0]], axis=axis)
    return lax.dot_general(lhs, rhs, dims, preferred_element_type=jnp.float32)


def quick(left, right, dims=NT):
    return three(split(left), split(right), dims)


def pack_kernel(place, matrix, factor, *rest):
    pieces, (buffer, sems) = rest[:SLABS], rest[SLABS:]

    @pl.when(place[2] == 0)
    def _():
        copies = {}
        for tile in range(4):
            for m, source in enumerate((matrix, factor)):
                rows = pl.ds(tile * 8 * NB, 8 * NB)
                copies[tile, m] = pltpu.make_async_copy(source.at[rows], buffer.at[m, rows], sems.at[m * 4 + tile])
                copies[tile, m].start()
        for tile in range(4):
            for m in range(2):
                copies[tile, m].wait()
                for half in range(2):
                    for slab in range(SLABS):
                        value = buffer[m, pl.ds((tile * NB + slab * SLAB) * 8 + half, SLAB, stride=8), :]
                        pieces[slab][pl.ds(((m * 4 + tile) * 2 + half) * SLAB, SLAB), :] = value


def pack(place, matrix, factor):
    return pl.pallas_call(
        pack_kernel,
        in_specs=[pl.BlockSpec(memory_space=pltpu.SMEM)] + [pl.BlockSpec(memory_space=pltpu.HBM)] * 2,
        out_specs=[pl.BlockSpec(memory_space=pltpu.VMEM)] * SLABS,
        out_shape=[jax.ShapeDtypeStruct((16 * SLAB, 128), jnp.float32)] * SLABS,
        scratch_shapes=[pltpu.VMEM((2, 8192, 128), jnp.float32), pltpu.SemaphoreType.DMA((8,))],
        compiler_params=pltpu.CompilerParams(vmem_limit_bytes=40 * 2**20),
        name="pack",
    )(place, far(matrix), far(factor))


def iotas():
    return (
        lax.broadcasted_iota(jnp.int32, (NB, NB), 0),
        lax.broadcasted_iota(jnp.int32, (NB, NB), 1),
    )


def inverses(lowers):
    half = NB // 2
    rows = lax.broadcasted_iota(jnp.int32, (half, NB), 0)
    cols = lax.broadcasted_iota(jnp.int32, (half, NB), 1) % half
    eye = rows == cols
    left = lax.broadcasted_iota(jnp.int32, (half, NB), 1) < half

    def spread(value):
        return jnp.concatenate([jnp.where(left, value, 0.0), jnp.where(left, 0.0, value)], axis=0)

    compact = [jnp.concatenate([lower[:half, :half], lower[half:, half:]], axis=1) for lower in lowers]
    first = []
    for value in compact:
        diagonal = jnp.where(eye, value, 0.0)
        across = 1.0 / jnp.sum(diagonal, axis=0, keepdims=True)
        down = [1.0 / jnp.sum(jnp.where(side, diagonal, 0.0), axis=1, keepdims=True) for side in (left, ~left)]
        down = jnp.where(left, down[0], down[1])
        pair = (rows // 2 == cols // 2) & (rows > cols)
        first.append(jnp.where(eye, across, 0.0) - jnp.where(pair, value * down * across, 0.0))

    def double(level, values):
        step = jnp.right_shift(rows, level) - jnp.right_shift(cols, level)
        band = (step == 1) & (jnp.right_shift(rows, level + 1) == jnp.right_shift(cols, level + 1))
        blocks = [quick(value, spread(jnp.where(band, whole, 0.0)), NN) for value, whole in zip(values, compact)]
        return tuple(value - quick(block, spread(value), NN) for value, block in zip(values, blocks))

    values = tuple(first)
    for level in range(1, 7):
        values = double(level, values)
    out = []
    for value, lower in zip(values, lowers):
        top, low = value[:, :half], value[:, half:]
        corner = quick(quick(low, lower[half:, :half], NN), top, NN)
        result = jnp.concatenate([jnp.where(left, value, 0.0), jnp.concatenate([-corner, low], axis=1)], axis=0)
        diag_rows, diag_cols = iotas()
        rest = jnp.where(diag_rows == diag_cols, 1.0, 0.0) - full(lower, result, NN)
        out.append(result + quick(result, rest, NN))
    return out


def head_math(tile, head_hi, head_lo, cores):
    a00, l00, a10, low, a11, l11 = (tile(*k) for k in ((0, 0, 0), (0, 0, 1), (0, 1, 0), (0, 1, 1), (1, 1, 0), (1, 1, 1)))
    rows, cols = iotas()
    eye = rows == cols

    def keep(k, value):
        head_hi[k], head_lo[k] = split(value)
        return head_hi[k], head_lo[k]

    inv0, inv1 = inverses((l00, l11))
    inv0, inv1, low = keep(0, inv0), keep(2, inv1), keep(5, low)
    part = three(split(three(inv0, split(jnp.where(eye, 0.5 * a00, a00)), NN)), inv0)
    cores[0] = part + part.T
    shared = three(low, keep(1, cores[0]))
    half0 = three(split(a10), inv0) - 0.5 * shared
    keep(4, half0 - 0.5 * shared)
    inner = jnp.where(eye, 0.5 * a11, a11) - three(split(half0), low)
    part = three(split(three(inv1, split(inner), NN)), inv1)
    cores[1] = part + part.T
    keep(3, cores[1])


def main_kernel(place, raw_far, local_far, *rest):
    grids, rest = rest[:10], rest[10:]
    out, raw_row, raw_col, local, head, cores, col_hi, col_lo, row_hi, row_lo, halves, head_hi, head_lo, sems = rest
    step = pl.program_id(0)
    p = place[0]
    c = place[1]

    def load_local(tile):
        return pltpu.make_async_copy(local_far.at[pl.ds(tile * 2048, 2048)], local.at[tile], sems.at[tile])

    def read(raw, core, m, pair):
        tiles = []
        for k in range(2):
            at = (m * 4 + pair * 2 + k) * 2
            tiles.append(jnp.concatenate([raw[:, core, at + half].reshape(NB, 128) for half in range(2)], axis=1))
        return jnp.concatenate(tiles, axis=0)

    def heads(k):
        return head_hi[k], head_lo[k]

    def keep(high, low, pair, k, value):
        for t in range(2):
            high[pair * 2 + t, :, k * NB : (k + 1) * NB] = value[0][t * NB : (t + 1) * NB]
            low[pair * 2 + t, :, k * NB : (k + 1) * NB] = value[1][t * NB : (t + 1) * NB]

    def panels(raw, tile):
        f0, f1 = split(read(raw, 0, 1, tile)), split(read(raw, 1, 1, tile))
        half0 = three(split(read(raw, 0, 0, tile)), heads(0))
        g0 = split(half0)
        a1 = read(raw, 1, 0, tile) - three(g0, heads(5)) - three(f0, heads(4))
        half1 = three(split(a1), heads(2))
        return half0, f0, half1, f1, g0

    @pl.when(step == 0)
    def _():
        load_row = pltpu.make_async_copy(raw_far.at[:, :, pl.ds(0, 16)], raw_row, sems.at[4])
        load_head = pltpu.make_async_copy(raw_far.at[:, :, pl.ds(16, 8)], head, sems.at[5])
        load_head.start()
        y, x = p // 4, p % 4
        loads = []

        def spot(dy, dx):
            return (((y + dy) % 4) * 4 + (x + dx) % 4 + 16 - c) % 16

        for m in range(2):
            near, back, ahead, far_one, far_two = grids[5 * m : 5 * m + 5]
            order = (0, 3, 1, 2)
            for k in range(4):
                for part, dy in ((near, 0), (back, 3), (ahead, 1), (far_one if k < 2 else far_two, 2)):
                    dx = order[k]
                    at = spot(dy, dx) if m == 0 else spot(dx, dy)
                    if dy == 2:
                        slot = raw_col.at[at // 2, at % 2, pl.ds(8 * m, 8)]
                        loads.append(pltpu.make_async_copy(part.at[k % 2], slot, sems.at[6 + 4 * m + k]))
                        loads[-1].start()
                    else:
                        raw_col[at // 2, at % 2, 8 * m : 8 * m + 8] = part[k]
        load_head.wait()
        load_row.start()
        for tile in range(4):
            load_local(tile).start()

        def square(core, row, m):
            at = (row * 2 + m) * 2
            return jnp.concatenate([head[:, core, at + half].reshape(NB, 128) for half in range(2)], axis=1)

        head_math(square, head_hi, head_lo, cores)
        for load in loads:
            load.wait()

        load_row.wait()

        def one(pair, carry):
            half0, f0, half1, f1, _ = panels(raw_col, pair)
            g0 = split(half0 - three(f0, heads(1)))
            g1 = split(half1 - three(f1, heads(3)))
            for k, value in enumerate((f0, g0, f1, g1)):
                keep(col_hi, col_lo, pair, k, value)
            half0, f0, half1, f1, g0 = panels(raw_row, pair)
            for k, value in enumerate((g0, f0, split(half1), f1)):
                keep(row_hi, row_lo, pair, k, value)
            for k, value in enumerate((half0, half1)):
                for t in range(2):
                    halves[k, pair * 2 + t] = value[t * NB : (t + 1) * NB]
            return carry

        lax.fori_loop(0, 2, one, 0)

    load_local(step).wait()
    rows, cols = iotas()

    def put(tile, value):
        for half in range(2):
            out[pl.ds(tile * 2 + half, NB, stride=8), :] = value[:, half * 128 : (half + 1) * 128]

    def get(tile):
        return jnp.concatenate([local[step, pl.ds(tile * 2 + half, NB, stride=8), :] for half in range(2)], axis=1)

    def update(tile, carry):
        below = (step > tile) | ((step == tile) & (p > c))
        same = (step == tile) & (p == c)
        ours = (below | same) & ((tile > 0) | (c > 1))

        @pl.when(ours)
        def _():
            change = three((row_hi[step], row_lo[step]), (col_hi[tile], col_lo[tile]))
            keep = jnp.logical_or(below, rows >= cols)
            put(tile, get(tile) - jnp.where(keep, change, 0.0))

        @pl.when(jnp.logical_not(ours))
        def _():
            put(tile, get(tile))

        return carry

    lax.fori_loop(0, 4, update, 0)
    top = step * 16 + p
    for block in range(2):

        @pl.when((c == block) & (top > block))
        def _():
            lanes = slice((2 * block + 1) * NB, (2 * block + 2) * NB)
            f = row_hi[step, :, lanes], row_lo[step, :, lanes]
            put(0, halves[block, step] - three(f, heads(2 * block + 1)))

        @pl.when((c == block) & (top == block))
        def _():
            put(0, jnp.where(rows >= cols, cores[block], 0.0))


def main_math(place, raw_row, grids, local):
    raw = (SLABS, 2, 16, SLAB, 128)
    vmem = pl.BlockSpec(memory_space=pltpu.VMEM)
    hbm = pl.BlockSpec(memory_space=pltpu.HBM)
    grids = [part.reshape(-1, 8, SLAB, 128) for part in grids]
    grids = [far(part) if k % 5 > 2 else part for k, part in enumerate(grids)]
    places = [hbm if k % 5 > 2 else vmem for k in range(10)]
    return pl.pallas_call(
        main_kernel,
        grid=(4,),
        in_specs=[pl.BlockSpec(memory_space=pltpu.SMEM), hbm, hbm] + places,
        out_specs=pl.BlockSpec((2048, 128), lambda i: (i, 0)),
        out_shape=jax.ShapeDtypeStruct((8192, 128), jnp.float32),
        scratch_shapes=[
            pltpu.VMEM(raw, jnp.float32),
            pltpu.VMEM(raw, jnp.float32),
            pltpu.VMEM((4, 2048, 128), jnp.float32),
            pltpu.VMEM((SLABS, 2, 8, SLAB, 128), jnp.float32),
            pltpu.VMEM((2, NB, NB), jnp.float32),
            pltpu.VMEM((4, NB, 4 * NB), jnp.bfloat16),
            pltpu.VMEM((4, NB, 4 * NB), jnp.bfloat16),
            pltpu.VMEM((4, NB, 4 * NB), jnp.bfloat16),
            pltpu.VMEM((4, NB, 4 * NB), jnp.bfloat16),
            pltpu.VMEM((2, 4, NB, NB), jnp.float32),
            pltpu.VMEM((6, NB, NB), jnp.bfloat16),
            pltpu.VMEM((6, NB, NB), jnp.bfloat16),
            pltpu.SemaphoreType.DMA((14,)),
        ],
        compiler_params=pltpu.CompilerParams(vmem_limit_bytes=40 * 2**20),
        name="main",
    )(place, far(raw_row.reshape(SLABS, 2, 24, SLAB, 128)), far(local), *grids)


def shift(value, axis, size, by):
    return lax.ppermute(value, axis, [(i, (i + by) % size) for i in range(size)])


def near4(value, axis):
    return [value] + [shift(value, axis, 4, by) for by in (1, -1, 2)]


def far(value):
    return pltpu.with_memory_space_constraint(value, pltpu.HBM)


def ring4(value, axis):
    up, down = shift(value, axis, 4, 1), shift(value, axis, 4, -1)
    half = value.shape[0] // 2
    return [value, up, down, shift(up[:half], axis, 4, 1), shift(down[half:], axis, 4, -1)]


def device(matrix, factor):
    x, y, z, _ = (lax.axis_index(name) for name in ("x", "y", "z", "core"))
    p = lax.axis_index(ROW)
    c = lax.axis_index(COL)
    place = jnp.stack([p, c, z])
    local = matrix.reshape(8192, 128)
    pieces = pack(place, local, factor.reshape(8192, 128))
    order = (4, 1, 7, 2, 6, 3, 5)
    got = [lax.ppermute(pieces[k], "z", [(0, k)]) for k in order]
    total = got[0]
    for value in got[1:]:
        total = total + value
    mine = jnp.where(z == 0, pieces[0], total)
    moved = lax.ppermute(mine, ROW + COL, [(r * 16 + j, (j + r) % 16 * 16 + j) for r in range(16) for j in range(16)])
    swapped = lax.ppermute(moved, ROW + COL, [(q * 16 + j, q * 16 + (q - j) % 16) for q in range(16) for j in range(16)])

    top = mine.reshape(2, 4, 2 * SLAB, 128)[:, 0].reshape(4 * SLAB, 128)
    across = lax.ppermute(top, ROW, [(0, 1), (1, 0)])
    tops = jnp.concatenate([jnp.where(p == 0, top, across), jnp.where(p == 0, across, top)], 0)
    sent = lax.ppermute(tops, ROW, [(0, 3), (1, 2)])
    tops = jnp.where(x < 2, tops, sent)
    sent = [lax.ppermute(tops, "y", [(0, k)]) for k in (2, 1, 3)]
    tops = jnp.where(y == 0, tops, sent[0] + sent[1] + sent[2])
    raw_row = lax.all_gather(jnp.concatenate([mine, tops], 0), COL)

    first = near4(swapped[: 8 * SLAB], "x")
    second = near4(swapped[8 * SLAB :], "y")
    grids = ring4(jnp.concatenate(first, 0), "y") + ring4(jnp.concatenate(second, 0), "x")
    return main_math(place, raw_row, grids, local).reshape(matrix.shape)


def solution(mesh):
    torus = Mesh(mesh.devices.reshape(4, 4, 8, 2), ("y", "x", "z", "core"))
    spec = P(None, ROW, None, None, COL, None)
    return jax.shard_map(device, mesh=torus, in_specs=(spec, spec), out_specs=spec, check_vma=False)
```
